128 devices in a mesh: tm: 4 (over x), feed: 32 (over y, z, core).
Axes of the slice: x: 4, y: 4, z: 4, core: 2. Of those that a mesh axis runs over, the one named last changes fastest.
Arguments:
- voltages: bfloat16 [2048, 98304], P('feed', 'tm'), may hold values from -6 to 6
- gains: bfloat16 [2, 2048, 1024], P(None, 'feed'), may hold values from -4 to 4
- beam_weights: bfloat16 [2, 2048, 2048], replicated, may hold values from -0.09375 to 0.09375
- delay_filter: float32 [1024, 1024], replicated, may hold values from -0.21875 to 0.21875
- channel_lists: int32 [32, 48], replicated, may hold values from -1 to 1023, as said below
- beam_order: int32 [2048], replicated, may hold values from 0 to 2047, each once
Outputs:
- filtered: float32 [4, 2048, 1024], P('tm', 'feed')
The draws below stay inside these ranges and needn't reach their ends.
Inputs may be any that keep to these rules, and one draw needn't show every extreme that they name: `channel_lists`: each row holds distinct channel numbers in its first places and -1 in the rest; 768 channel numbers are listed in all, none twice; a row lists 0 to 48 channels, and some row lists exactly 48.
All inputs are finite; a program needn't handle non-finite values.
Results may differ from the reference program's by a relative error of at most 0.0021.
Values may be sent and summed in bfloat16 or wider, within the bound.
No kernel may reach another device: no remote copies, remote signals or barrier semaphores. Data moves between devices by JAX's collectives and lax.ppermute only.
A program may use at most 192 MiB of HBM per device.

```python
import jax
import jax.numpy as jnp
from jax import lax

INPUTS = 2048
FFT = 2048
BEAMS = 2048
FR = 12
CHANNELS = 1024
LIVE = 768
SAMPLES = 98304
N_TM = 4
N_FEED = 32


def draw_channel_lists(key, part):
    even_share = LIVE // N_FEED
    capacity = 2 * even_share
    selected = jax.random.permutation(jax.random.fold_in(key, 11), CHANNELS)[:LIVE].astype(jnp.int32)
    shuffled = jax.random.permutation(jax.random.fold_in(key, 12), N_FEED).astype(jnp.int32)
    transfer = jax.random.randint(jax.random.fold_in(key, 13), (N_FEED // 2,), 0, even_share + 1).astype(jnp.int32)
    transfer = transfer.at[0].set(even_share)
    row_counts = jnp.full((N_FEED,), even_share, jnp.int32)
    row_counts = row_counts.at[shuffled[0::2]].add(transfer)
    row_counts = row_counts.at[shuffled[1::2]].add(-transfer)
    row_starts = jnp.cumsum(row_counts) - row_counts
    positions = jnp.arange(capacity, dtype=jnp.int32)[None, :]
    source_place = jnp.clip(row_starts[:, None] + positions, 0, LIVE - 1)
    return jnp.where(positions < row_counts[:, None], selected[source_place], -1).astype(jnp.int32)


def block_levels(key, extent, cuts, low, top_value):
    def one(dim, shards_of):
        draws = jax.random.uniform(jax.random.fold_in(jax.random.fold_in(key, 6), dim), (shards_of,), jnp.float32, low / len(cuts), top_value / len(cuts))
        return jnp.repeat(jnp.exp(draws), extent[dim] // shards_of).reshape((-1,) + (1,) * (len(extent) - dim - 1))

    gain = one(*cuts[0])
    for cut in cuts[1:]:
        gain = gain * one(*cut)
    return gain


def gaussian(rng, dims, scale, most, cuts=(), kind=jnp.bfloat16):
    factor_of = block_levels(rng, dims, cuts, -0.22, 0.18) if cuts else 1.0
    array = jax.random.normal(rng, dims, jnp.float32) * scale * factor_of
    return jnp.minimum(jnp.maximum(array, -most), most).astype(kind)


def setup_inputs(seed: int = 0) -> dict:
    splits = jax.random.split(jax.random.key(seed), 7)
    return {
        "voltages": gaussian(splits[0], (INPUTS, SAMPLES), 1.0, 6.0, ((0, 32), (1, 4))),
        "gains": gaussian(splits[1], (2, INPUTS, CHANNELS), 0.7, 4.0, ((1, 32),)),
        "beam_weights": gaussian(splits[2], (2, BEAMS, INPUTS), (2 * INPUTS) ** -0.5, 0.09375),
        "delay_filter": gaussian(splits[3], (CHANNELS, CHANNELS), LIVE ** -0.5, 0.21875, (), jnp.float32),
        "channel_lists": draw_channel_lists(jax.random.fold_in(splits[6], 71), 0),
        "beam_order": jax.random.permutation(splits[5], BEAMS).astype(jnp.int32),
    }


def make_window(length):
    places = jnp.arange(4 * length, dtype=jnp.float32)
    centred = (places - 2.0 * length + 0.5) / length
    taper = 0.5 - 0.5 * jnp.cos(2.0 * jnp.pi * (places + 0.5) / (4.0 * length))
    return (jnp.sinc(centred) * taper).reshape(4, length)


def make_table(length):
    sample_rows = jnp.arange(length, dtype=jnp.int32)[:, None]
    channel_cols = jnp.arange(length // 2, dtype=jnp.int32)[None, :]
    phases = ((sample_rows * channel_cols) % length).astype(jnp.float32)
    angles = 2.0 * jnp.pi * phases / length
    scaling = length ** -0.5
    return jnp.concatenate([jnp.cos(angles) * scaling, -jnp.sin(angles) * scaling], axis=1).astype(jnp.bfloat16)


def filterbank(extended, window, dft_table, frame_count):
    weighted = window[0] * extended[:, 0:frame_count].astype(jnp.float32)
    for tap_index in range(1, 4):
        weighted = weighted + window[tap_index] * extended[:, tap_index:tap_index + frame_count].astype(jnp.float32)
    weighted = weighted.astype(jnp.bfloat16)
    rows = weighted.shape[0] * frame_count
    flat_rows = weighted.reshape(rows, weighted.shape[2]).astype(jnp.float32)
    spectra = jnp.dot(flat_rows, dft_table.astype(jnp.float32), preferred_element_type=jnp.float32)
    return spectra.reshape(weighted.shape[0], frame_count, dft_table.shape[1])


def reference(voltages, gains, beam_weights, delay_filter, channel_lists, beam_order):
    window = make_window(FFT)
    dft_table = make_table(FFT)
    flattened = channel_lists.reshape(-1)
    listed = flattened >= 0
    safe_ids = jnp.where(listed, flattened, 0).astype(jnp.int32)
    live_mask = jnp.zeros((CHANNELS,), jnp.float32).at[safe_ids].add(listed.astype(jnp.float32))
    weights = beam_weights.reshape(2 * BEAMS, INPUTS).astype(jnp.float32)
    all_frames = voltages.reshape(INPUTS, N_TM, FR, FFT)
    gain_real = gains[0].astype(jnp.float32)[:, None, :]
    gain_imag = gains[1].astype(jnp.float32)[:, None, :]
    columns = CHANNELS * FR
    results = []
    for block_index in range(N_TM):
        if block_index == 0:
            earlier = jnp.zeros((INPUTS, 3, FFT), jnp.bfloat16)
        else:
            earlier = all_frames[:, block_index - 1, FR - 3:]
        extended = jnp.concatenate([earlier, all_frames[:, block_index]], axis=1)
        spectra = filterbank(extended, window, dft_table, FR)
        real_part = spectra[:, :, :CHANNELS]
        imag_part = spectra[:, :, CHANNELS:]
        gained_real = (real_part * gain_real - imag_part * gain_imag).astype(jnp.bfloat16)
        gained_imag = (real_part * gain_imag + imag_part * gain_real).astype(jnp.bfloat16)
        stacked = jnp.stack([gained_real, gained_imag], axis=1)
        stacked = jnp.transpose(stacked, (0, 1, 3, 2)).reshape(INPUTS, 2 * columns)
        product = jnp.dot(weights, stacked.astype(jnp.float32), preferred_element_type=jnp.float32)
        beams_real = product[:BEAMS, :columns] - product[BEAMS:, columns:]
        beams_imag = product[:BEAMS, columns:] + product[BEAMS:, :columns]
        powers = (beams_real * beams_real + beams_imag * beams_imag).reshape(BEAMS, CHANNELS, FR)
        powers = jnp.mean(powers, axis=2)
        masked = powers * live_mask[None, :]
        filtered = jnp.dot(masked, delay_filter, precision=lax.Precision.HIGHEST, preferred_element_type=jnp.float32)
        results.append(filtered[beam_order])
    return jnp.stack(results, axis=0)
```

```python
import functools

import jax
import jax.numpy as jnp
import numpy as np
from jax import lax
from jax.experimental import pallas as pl
from jax.experimental.pallas import tpu as pltpu
from jax.sharding import PartitionSpec as P

FFT = 2048
BEAMS = 2048
CHANNELS = 1024
LIVE = 768
FR = 12
LATE = 4
NT = (((1,), (1,)), ((), ()))
TN = (((0,), (0,)), ((), ()))
F32 = jnp.float32
BF16 = jnp.bfloat16


def make_window(length):
    places = np.arange(4 * length, dtype=np.float64)
    centred = (places - 2.0 * length + 0.5) / length
    taper = 0.5 - 0.5 * np.cos(2.0 * np.pi * (places + 0.5) / (4.0 * length))
    return (np.sinc(centred) * taper).reshape(4, length).astype(np.float32)


def cos_sin(phase):
    quarter = lax.shift_right_logical(phase + 256, 9)
    x = (phase - quarter * 512).astype(F32) * np.float32(np.pi / 1024)
    y = x * x
    s = x * (1.0 + y * (-1.0 / 6 + y * (1.0 / 120 + y * (-1.0 / 5040 + y * (1.0 / 362880)))))
    c = 1.0 + y * (
        -0.5 + y * (1.0 / 24 + y * (-1.0 / 720 + y * (1.0 / 40320 + y * (-1.0 / 3628800))))
    )
    odd = (quarter & 1) == 1
    cos = jnp.where(odd, s, c)
    sin = jnp.where(odd, c, s)
    cos = jnp.where(((quarter + 1) & 2) == 2, -cos, cos)
    sin = jnp.where((quarter & 2) == 2, -sin, sin)
    return cos, sin


def slots_of(lists):
    groups, places = lists.shape
    listed = (lists >= 0).astype(F32)
    counts = jnp.sum(listed, axis=1, keepdims=True)
    above = lax.broadcasted_iota(jnp.int32, (groups, groups), 0)
    here = lax.broadcasted_iota(jnp.int32, (groups, groups), 1)
    wide = jnp.broadcast_to(counts, (groups, groups))
    first = jnp.sum(jnp.where(above < here, wide, 0.0), axis=0, keepdims=True)
    count = jnp.sum(jnp.where(above == here, wide, 0.0), axis=0, keepdims=True)
    slot = lax.broadcasted_iota(jnp.int32, (LIVE, groups), 0).astype(F32)
    inside = (slot >= first) & (slot < first + count)
    pick = jnp.where(inside, 1.0, 0.0)
    place = jnp.sum(jnp.where(inside, slot - first, 0.0), axis=1, keepdims=True)
    known = jnp.maximum(lists, 0)
    high = (known >> 5).astype(F32).astype(BF16)
    low = (known & 31).astype(F32).astype(BF16)
    pick = pick.astype(BF16)
    rows = 32.0 * jnp.dot(pick, high, preferred_element_type=F32) + jnp.dot(
        pick, low, preferred_element_type=F32
    )
    across = lax.broadcasted_iota(jnp.int32, (LIVE, places), 1).astype(F32)
    return jnp.sum(jnp.where(across == place, rows, 0.0), axis=1, keepdims=True)


def fir(read, window_ref, weighted_ref, count, inputs):
    def tile(step, carry):
        lane = pl.multiple_of(step * 128, 128)
        taps = [window_ref[pl.ds(t, 1), pl.ds(lane, 128)] for t in range(4)]
        for row in range(0, inputs, 16):
            frames = [read(f, row, lane).astype(F32) for f in range(count + 3)]
            for k in range(count):
                total = taps[0] * frames[k]
                for t in range(1, 4):
                    total = total + taps[t] * frames[k + t]
                weighted_ref[pl.ds(k * inputs + row, 16), pl.ds(lane, 128)] = total.astype(BF16)
        return carry

    lax.fori_loop(0, FFT // 128, tile, 0)


def spectra_and_gains(table_ref, weighted_ref, gain_ref, out_ref, groups, width):
    half = groups // 2
    rows = 2 * LIVE // 2
    share = LIVE // groups

    def part(step, carry):
        block = step % 2
        lane = pl.multiple_of((step // 2) * 256, 256)
        product = lax.dot_general(
            table_ref[pl.ds(pl.multiple_of(block * rows, rows), rows), :],
            weighted_ref[pl.ds(lane, 256), :],
            NT,
            preferred_element_type=F32,
        )
        for g in range(half):
            here = block * half + g
            at = pl.multiple_of(here * share, share)
            real_gain = gain_ref[pl.ds(at, share), 0:128]
            imag_gain = gain_ref[pl.ds(at, share), 128:256]
            for piece in range(2):
                cut = slice(piece * 128, piece * 128 + 128)
                real = product[g * 2 * share : g * 2 * share + share, cut]
                imag = product[g * 2 * share + share : (g + 1) * 2 * share, cut]
                both = jnp.concatenate(
                    [
                        real * real_gain - imag * imag_gain,
                        real * imag_gain + imag * real_gain,
                    ],
                    axis=0,
                )
                out_ref[here, :, pl.ds(lane + piece * 128, 128)] = both.astype(BF16)
        return carry

    lax.fori_loop(0, 2 * (width // 256), part, 0)


def early_kernel(
    lists_ref, gains_ref, window_ref, volts_ref,
    out_ref, table_ref, gain_ref, pick_ref, channel_ref, weighted_ref,
):
    groups = lists_ref.shape[0]
    inputs = volts_ref.shape[0]
    share = LIVE // groups
    channel_ref[...] = jnp.broadcast_to(slots_of(lists_ref[...]), (LIVE, 128)).astype(jnp.int32)

    def table_rows(g, carry):
        at = pl.multiple_of(g * share, share)
        channel = channel_ref[pl.ds(at, share), :]
        lane = lax.broadcasted_iota(jnp.int32, (share, 128), 1)
        cos, sin = cos_sin((channel * lane) & (FFT - 1))
        scale = np.float32(FFT ** (-0.5))
        real, imag = cos * scale, -sin * scale
        turn_cos, turn_sin = cos_sin((channel * 128) & (FFT - 1))
        for j in range(FFT // 128):
            both = jnp.concatenate([real, imag], axis=0).astype(BF16)
            table_ref[pl.ds(pl.multiple_of(g * 2 * share, 2 * share), 2 * share), j * 128 : (j + 1) * 128] = both
            real, imag = real * turn_cos + imag * turn_sin, imag * turn_cos - real * turn_sin
        for j in range(CHANNELS // 128):
            pick_ref[pl.ds(at, share), j * 128 : (j + 1) * 128] = jnp.where(
                channel == lane + j * 128, 1.0, 0.0
            ).astype(BF16)
        return carry

    lax.fori_loop(0, groups, table_rows, 0)
    gain = lax.dot_general(pick_ref[...], gains_ref[...], NT, preferred_element_type=F32)
    turned = pltpu.roll(gain, 64, 1)
    low = lax.broadcasted_iota(jnp.int32, gain.shape, 1) < 64
    gain_ref[:, 0:128] = jnp.where(low, gain, turned)
    gain_ref[:, 128:256] = jnp.where(low, turned, gain)

    def read(f, row, lane):
        return volts_ref[pl.ds(row, 16), pl.ds(lane + (f + LATE - 3) * FFT, 128)]

    count = FR - LATE
    fir(read, window_ref, weighted_ref, count, inputs)
    spectra_and_gains(table_ref, weighted_ref, gain_ref, out_ref, groups, count * inputs)


def late_kernel(table_ref, gain_ref, window_ref, before_ref, volts_ref, out_ref, weighted_ref):
    groups = out_ref.shape[0]
    inputs = volts_ref.shape[0]

    def read(f, row, lane):
        if f < 3:
            return before_ref[pl.ds(row, 16), pl.ds(lane + f * FFT, 128)]
        return volts_ref[pl.ds(row, 16), pl.ds(lane + (f - 3) * FFT, 128)]

    fir(read, window_ref, weighted_ref, LATE, inputs)
    spectra_and_gains(table_ref, weighted_ref, gain_ref, out_ref, groups, LATE * inputs)


def arrange(received_ref, spread_ref):
    groups, rows, width = received_ref.shape
    low = lax.broadcasted_iota(jnp.int32, (rows, 128), 1) < 64
    for pair in range(groups // 2):
        for two in range(width // 128):
            cut = slice(two * 128, two * 128 + 128)
            first = received_ref[2 * pair, :, cut].astype(F32)
            second = received_ref[2 * pair + 1, :, cut].astype(F32)
            one = jnp.where(low, first, pltpu.roll(second, 64, 1))
            other = jnp.where(low, pltpu.roll(first, 64, 1), second)
            at = slice(pair * 128, pair * 128 + 128)
            spread_ref[2 * two * rows : (2 * two + 1) * rows, at] = one.astype(BF16)
            spread_ref[(2 * two + 1) * rows : (2 * two + 2) * rows, at] = other.astype(BF16)


def beam_powers(spread_ref, weights_ref, rows):
    by_real = lax.dot_general(spread_ref[...], weights_ref[0], NT, preferred_element_type=F32)
    by_imag = lax.dot_general(spread_ref[...], weights_ref[1], NT, preferred_element_type=F32)
    half = rows // 2
    total = None
    for k in range(spread_ref.shape[0] // rows):
        top, middle, end = k * rows, k * rows + half, (k + 1) * rows
        real = by_real[top:middle] - by_imag[middle:end]
        imag = by_real[middle:end] + by_imag[top:middle]
        power = real * real + imag * imag
        total = power if total is None else total + power
    return total


def first_beams_kernel(received_ref, weights_ref, out_ref, spread_ref):
    @pl.when(pl.program_id(0) == 0)
    def _():
        arrange(received_ref, spread_ref)

    out_ref[...] = beam_powers(spread_ref, weights_ref, received_ref.shape[1])


def last_beams_kernel(
    received_ref, weights_ref, partial_ref, order_ref, out_ref, spread_ref, powers_ref
):
    step = pl.program_id(0)
    tiles = powers_ref.shape[0]
    per_step = out_ref.shape[0] // 2

    @pl.when(step == 0)
    def _():
        arrange(received_ref, spread_ref)

    total = partial_ref[...] + beam_powers(spread_ref, weights_ref, received_ref.shape[1])
    total = total * np.float32(1.0 / FR)
    here = total.shape[1] // 128
    for j in range(here):
        powers_ref[step * here + j] = total[:, j * 128 : (j + 1) * 128]

    @pl.when(step == pl.num_programs(0) - 1)
    def _():
        rows = powers_ref.shape[1]
        low = lax.broadcasted_iota(jnp.int32, (rows, 128), 1) < 64

        def move(tile, carry):
            order = jnp.broadcast_to(order_ref[pl.ds(tile, 1), :], (rows, 128))
            lane = order & 127
            source = order >> 7
            moved = jnp.zeros((rows, 128), F32)
            for j in range(tiles):
                moved = jnp.where(
                    source == j,
                    jnp.take_along_axis(powers_ref[j], lane, axis=1),
                    moved,
                )
            high = moved.astype(BF16).astype(F32)
            rest = moved - high
            out_ref[2 * tile] = jnp.where(low, high, pltpu.roll(rest, 64, 1)).astype(BF16)
            out_ref[2 * tile + 1] = jnp.where(low, pltpu.roll(high, 64, 1), rest).astype(BF16)
            return carry

        lax.fori_loop(0, tiles, move, 0)


def filter_rows_kernel(pick_ref, filter_ref, high_ref, low_ref):
    whole = filter_ref[...]
    high = whole.astype(BF16)
    low = (whole - high.astype(F32)).astype(BF16)
    high_ref[...] = jnp.dot(pick_ref[...], high, preferred_element_type=F32).astype(BF16)
    low_ref[...] = jnp.dot(pick_ref[...], low, preferred_element_type=F32).astype(BF16)


def filter_kernel(powers_ref, high_ref, low_ref, out_ref):
    powers = powers_ref[...]
    both = lax.dot_general(powers, high_ref[...], TN, preferred_element_type=F32)
    rest = lax.dot_general(powers, low_ref[...], TN, preferred_element_type=F32)
    half = out_ref.shape[0]
    out_ref[...] = (both[half:] + rest[:half]) + both[:half]


def cost(flops, data=0):
    return pl.CostEstimate(flops=int(flops), bytes_accessed=int(data), transcendentals=0)


def params(limit=None, **more):
    return pltpu.CompilerParams(vmem_limit_bytes=limit, **more)


VM = pl.BlockSpec(memory_space=pltpu.VMEM)


def body(voltages, gains, beam_weights, delay_filter, channel_lists, beam_order):
    groups = lax.axis_size("feed")
    steps = lax.axis_size("tm")
    inputs = voltages.shape[0]
    share = LIVE // groups
    mine = BEAMS // groups
    window = jnp.asarray(make_window(FFT))
    before = lax.ppermute(
        voltages[:, (FR - 3) * FFT :], "tm", [(i, i + 1) for i in range(steps - 1)]
    )
    early = (FR - LATE) * inputs
    late = LATE * inputs
    mib = 1 << 20
    spectra, table, gain, pick = pl.pallas_call(
        early_kernel,
        out_shape=(
            jax.ShapeDtypeStruct((groups, 2 * share, early), BF16),
            jax.ShapeDtypeStruct((2 * LIVE, FFT), BF16),
            jax.ShapeDtypeStruct((LIVE, 256), F32),
            jax.ShapeDtypeStruct((LIVE, CHANNELS), BF16),
        ),
        in_specs=[VM] * 4,
        out_specs=(VM,) * 4,
        scratch_shapes=[pltpu.VMEM((LIVE, 128), jnp.int32), pltpu.VMEM((early, FFT), BF16)],
        compiler_params=params(40 * mib),
        cost_estimate=cost(2 * 2 * LIVE * FFT * early),
        name="early",
    )(channel_lists, gains.reshape(2 * inputs, CHANNELS), window, voltages)
    first = lax.all_to_all(spectra, "feed", split_axis=0, concat_axis=0, tiled=True)
    spectra = pl.pallas_call(
        late_kernel,
        out_shape=jax.ShapeDtypeStruct((groups, 2 * share, late), BF16),
        grid=(1,),
        in_specs=[
            VM, VM, VM, VM,
            pl.BlockSpec((inputs, LATE * FFT), lambda i: (0, 0)),
        ],
        out_specs=VM,
        scratch_shapes=[pltpu.VMEM((late, FFT), BF16)],
        compiler_params=params(40 * mib),
        cost_estimate=cost(2 * 2 * LIVE * FFT * late),
        name="late",
    )(table, gain, window, before, voltages)
    filter_high, filter_low = pl.pallas_call(
        filter_rows_kernel,
        out_shape=(jax.ShapeDtypeStruct((LIVE, CHANNELS), BF16),) * 2,
        in_specs=[VM] * 2,
        out_specs=(VM,) * 2,
        compiler_params=params(40 * mib),
        cost_estimate=cost(4 * LIVE * CHANNELS * CHANNELS),
        name="filter_rows",
    )(pick, delay_filter)
    second = lax.all_to_all(spectra, "feed", split_axis=0, concat_axis=0, tiled=True)
    span = 256
    partial = pl.pallas_call(
        first_beams_kernel,
        out_shape=jax.ShapeDtypeStruct((share, BEAMS), F32),
        grid=(BEAMS // span,),
        in_specs=[VM, pl.BlockSpec((2, span, groups * inputs), lambda i: (0, i, 0))],
        out_specs=pl.BlockSpec((share, span), lambda i: (0, i)),
        scratch_shapes=[pltpu.VMEM((2 * share * (FR - LATE), groups * inputs), BF16)],
        compiler_params=params(40 * mib),
        cost_estimate=cost(2 * 2 * BEAMS * groups * inputs * 2 * share * (FR - LATE)),
        name="first_beams",
    )(first, beam_weights)
    powers = pl.pallas_call(
        last_beams_kernel,
        out_shape=jax.ShapeDtypeStruct((groups, share, 2 * mine), BF16),
        grid=(BEAMS // span,),
        in_specs=[
            VM,
            pl.BlockSpec((2, span, groups * inputs), lambda i: (0, i, 0)),
            pl.BlockSpec((share, span), lambda i: (0, i)),
            VM,
        ],
        out_specs=pl.BlockSpec((groups, share, 2 * mine), lambda i: (0, 0, 0)),
        scratch_shapes=[
            pltpu.VMEM((2 * share * LATE, groups * inputs), BF16),
            pltpu.VMEM((BEAMS // 128, share, 128), F32),
        ],
        compiler_params=params(40 * mib),
        cost_estimate=cost(2 * 2 * BEAMS * groups * inputs * 2 * share * LATE),
        name="last_beams",
    )(second, beam_weights, partial, beam_order.reshape(BEAMS // 128, 128))
    owned = lax.all_to_all(powers, "feed", split_axis=0, concat_axis=0, tiled=True)
    filtered = pl.pallas_call(
        filter_kernel,
        out_shape=jax.ShapeDtypeStruct((mine, CHANNELS), F32),
        in_specs=[VM] * 3,
        out_specs=VM,
        compiler_params=params(40 * mib),
        cost_estimate=cost(4 * LIVE * CHANNELS * 2 * mine),
        name="filter",
    )(owned.reshape(LIVE, 2 * mine), filter_high, filter_low)
    return filtered.reshape(1, mine, CHANNELS)


def solution(mesh):
    placed = (P("feed", "tm"), P(None, "feed", None), P(), P(), P(), P())
    return jax.shard_map(
        body, mesh=mesh, in_specs=placed, out_specs=P("tm", "feed", None), check_vma=False
    )
```

```python
import functools

import jax
import jax.numpy as jnp
import numpy as np
from jax import lax
from jax.experimental import pallas as pl
from jax.experimental.pallas import tpu as pltpu
from jax.sharding import PartitionSpec as P


FFT = 2048
BEAMS = 2048
CHANNELS = 1024
LIVE = 768
FR = 12
LATE = 4
NT = (((1,), (1,)), ((), ()))
TN = (((0,), (0,)), ((), ()))
F32 = jnp.float32
BF16 = jnp.bfloat16


def make_window(length):
    places = np.arange(4 * length, dtype=np.float64)
    centred = (places - 2.0 * length + 0.5) / length
    taper = 0.5 - 0.5 * np.cos(2.0 * np.pi * (places + 0.5) / (4.0 * length))
    return (np.sinc(centred) * taper).reshape(4, length).astype(np.float32)


def cos_sin(phase):
    quarter = lax.shift_right_logical(phase + 256, 9)
    x = (phase - quarter * 512).astype(F32) * np.float32(np.pi / 1024)
    y = x * x
    s = x * (1.0 + y * (-1.0 / 6 + y * (1.0 / 120 + y * (-1.0 / 5040 + y * (1.0 / 362880)))))
    c = 1.0 + y * (
        -0.5 + y * (1.0 / 24 + y * (-1.0 / 720 + y * (1.0 / 40320 + y * (-1.0 / 3628800))))
    )
    odd = (quarter & 1) == 1
    cos = jnp.where(odd, s, c)
    sin = jnp.where(odd, c, s)
    cos = jnp.where(((quarter + 1) & 2) == 2, -cos, cos)
    sin = jnp.where((quarter & 2) == 2, -sin, sin)
    return cos, sin


def slots_of(lists):
    groups, places = lists.shape
    both = 2 * groups
    odd = (lists & 1) == 1
    evens = jnp.where((lists >= 0) & ~odd, 1.0, 0.0)
    odds = jnp.where((lists >= 0) & odd, 1.0, 0.0)
    marks = jnp.concatenate([evens, odds], axis=0)
    ahead = lax.broadcasted_iota(jnp.int32, (places, places), 0)
    place = lax.broadcasted_iota(jnp.int32, (places, places), 1)
    earlier = jnp.where(ahead < place, 1.0, 0.0).astype(BF16)
    rank = jnp.dot(marks.astype(BF16), earlier, preferred_element_type=F32)
    keys = jnp.where(marks > 0.0, rank, -1.0).astype(BF16)
    counts = jnp.sum(marks, axis=1, keepdims=True)
    above = lax.broadcasted_iota(jnp.int32, (both, both), 0)
    here = lax.broadcasted_iota(jnp.int32, (both, both), 1)
    wide = jnp.broadcast_to(counts, (both, both))
    first = jnp.sum(jnp.where(above < here, wide, 0.0), axis=0, keepdims=True)
    count = jnp.sum(jnp.where(above == here, wide, 0.0), axis=0, keepdims=True)
    slot = lax.broadcasted_iota(jnp.int32, (LIVE, both), 0).astype(F32)
    inside = (slot >= first) & (slot < first + count)
    pick = jnp.where(inside, 1.0, 0.0).astype(BF16)
    wanted = jnp.sum(jnp.where(inside, slot - first, 0.0), axis=1, keepdims=True)
    known = jnp.maximum(lists, 0)
    known = jnp.concatenate([known, known], axis=0)
    high = (known >> 5).astype(F32).astype(BF16)
    low = (known & 31).astype(F32).astype(BF16)
    rows = 32.0 * jnp.dot(pick, high, preferred_element_type=F32) + jnp.dot(
        pick, low, preferred_element_type=F32
    )
    key = jnp.dot(pick, keys, preferred_element_type=F32)
    return jnp.sum(jnp.where(key == wanted, rows, 0.0), axis=1, keepdims=True)


def fir(read, window_ref, weighted_ref, count, inputs):
    half = FFT // 2

    def totals(row, lane):
        taps = [window_ref[pl.ds(t, 1), pl.ds(lane, 128)] for t in range(4)]
        frames = [read(f, row, lane).astype(F32) for f in range(count + 3)]
        out = []
        for k in range(count):
            total = taps[0] * frames[k]
            for t in range(1, 4):
                total = total + taps[t] * frames[k + t]
            out.append(total)
        return out

    def tile(step, carry):
        lane = pl.multiple_of(step * 128, 128)
        for row in range(0, inputs, 16):
            near = totals(row, lane)
            far = totals(row, lane + half)
            for k in range(count):
                at = pl.ds(k * inputs + row, 16)
                weighted_ref[at, pl.ds(lane, 128)] = (near[k] + far[k]).astype(BF16)
                weighted_ref[at, pl.ds(lane + half, 128)] = (near[k] - far[k]).astype(BF16)
        return carry

    lax.fori_loop(0, half // 128, tile, 0)


def spectra_and_gains(table_ref, weighted_ref, gain_ref, sign_ref, groups, width, store):
    share = LIVE // groups
    size = 2 * share
    pure = (LIVE - CHANNELS // 2) // share
    half = FFT // 2

    def part(step, carry):
        lane = pl.multiple_of(step * 256, 256)
        evens = lax.dot_general(
            table_ref[0 : (groups - pure) * size, :],
            weighted_ref[pl.ds(lane, 256), 0:half],
            NT,
            preferred_element_type=F32,
        )
        odds = lax.dot_general(
            table_ref[pure * size :, :],
            weighted_ref[pl.ds(lane, 256), half:FFT],
            NT,
            preferred_element_type=F32,
        )
        for g in range(groups):
            own = slice(g * share, (g + 1) * share)
            real_gain = gain_ref[own, 0:128]
            imag_gain = gain_ref[own, 128:256]
            even = sign_ref[own, :] > 0.0
            for piece in range(2):
                cut = slice(piece * 128, piece * 128 + 128)
                if g < groups - pure:
                    real = evens[g * size : g * size + share, cut]
                    imag = evens[g * size + share : (g + 1) * size, cut]
                if g >= pure:
                    at = (g - pure) * size
                    odd_real = odds[at : at + share, cut]
                    odd_imag = odds[at + share : at + size, cut]
                    if g < groups - pure:
                        real = jnp.where(even, real, odd_real)
                        imag = jnp.where(even, imag, odd_imag)
                    else:
                        real, imag = odd_real, odd_imag
                both = jnp.concatenate(
                    [
                        real * real_gain - imag * imag_gain,
                        real * imag_gain + imag * real_gain,
                    ],
                    axis=0,
                )
                store(g, lane + piece * 128, both.astype(BF16))
            if (g + 1) % SENT == 0:
                store(g, lane, None)
        return carry

    lax.fori_loop(0, width // 256, part, 0)


SENT = 8


def sender(out_vmem, out_hbm, sem):

    def copy(g, lane):
        at = (slice(g + 1 - SENT, g + 1), slice(None), pl.ds(lane, 256))
        return pltpu.make_async_copy(out_vmem.at[at], out_hbm.at[at], sem)

    def store(g, lane, value):
        if value is None:
            copy(g, lane).start()
        else:
            out_vmem[g, :, pl.ds(lane, 128)] = value

    def finish():
        pltpu.make_async_copy(out_vmem, out_hbm, sem).wait()

    return store, finish


def gain_loads(gains_hbm, gains_ref, sems):
    rows, half = gains_hbm.shape[0], CHANNELS // 2
    return [
        pltpu.make_async_copy(
            gains_hbm.at[:, part * half : (part + 1) * half],
            gains_ref.at[part * rows : (part + 1) * rows, :],
            sems.at[part],
        )
        for part in range(2)
    ]


def live_tables(
    lists_ref, channel_ref, table_ref, sign_ref, half_ref, gains_ref, gain_ref, ready, pick_ref=None
):
    groups = lists_ref.shape[0]
    share = LIVE // groups
    channel_ref[...] = jnp.broadcast_to(slots_of(lists_ref[...]), (LIVE, 128)).astype(jnp.int32)

    def table_rows(pair, carry):
        at = pl.multiple_of(pair * 2 * share, 2 * share)
        channel = channel_ref[pl.ds(at, 2 * share), :]
        lane = lax.broadcasted_iota(jnp.int32, channel.shape, 1)
        cos, sin = cos_sin((channel * lane) & (FFT - 1))
        scale = np.float32(FFT ** (-0.5))
        real, imag = cos * scale, -sin * scale
        half_cos = jnp.broadcast_to(cos[:, 64:65], cos.shape)
        half_sin = jnp.broadcast_to(sin[:, 64:65], sin.shape)
        turn_cos = 2.0 * half_cos * half_cos - 1.0
        turn_sin = 2.0 * half_cos * half_sin
        twice = 2.0 * turn_cos
        last = None
        row = pl.multiple_of(pair * 4 * share, 4 * share)
        for j in range(FFT // 256):
            both = jnp.concatenate(
                [real[:share], imag[:share], real[share:], imag[share:]], axis=0
            )
            table_ref[pl.ds(row, 4 * share), j * 128 : (j + 1) * 128] = both.astype(BF16)
            if last is None:
                following = (
                    real * turn_cos + imag * turn_sin,
                    imag * turn_cos - real * turn_sin,
                )
            else:
                following = (twice * real - last[0], twice * imag - last[1])
            last = (real, imag)
            real, imag = following
        sign_ref[pl.ds(at, 2 * share), :] = jnp.where((channel & 1) == 1, -1.0, 1.0)
        lower = channel & (CHANNELS // 2 - 1)
        picks = [(half_ref, lower, CHANNELS // 2)]
        if pick_ref is not None:
            picks.append((pick_ref, channel, CHANNELS))
        for ref, wanted, width in picks:
            for j in range(width // 128):
                ref[pl.ds(at, 2 * share), j * 128 : (j + 1) * 128] = jnp.where(
                    wanted == lane + j * 128, 1.0, 0.0
                ).astype(BF16)
        return carry

    lax.fori_loop(0, groups // 2, table_rows, 0)
    ready()
    either = lax.dot_general(half_ref[...], gains_ref[...], NT, preferred_element_type=F32)
    upper = channel_ref[...] >= CHANNELS // 2
    gain = jnp.where(upper, either[:, 128:256], either[:, 0:128])
    turned = pltpu.roll(gain, 64, 1)
    low = lax.broadcasted_iota(jnp.int32, gain.shape, 1) < 64
    gain_ref[:, 0:128] = jnp.where(low, gain, turned)
    gain_ref[:, 128:256] = jnp.where(low, turned, gain)


def early_kernel(
    lists_hbm, gains_hbm, window_hbm, volts_hbm, out_hbm, tail_hbm,
    lists_ref, gains_ref, window_ref, volts_ref, out_ref, table_ref, gain_ref, sign_ref, half_ref,
    channel_ref, weighted_ref, in_sems, out_sem, tail_sem,
):
    groups = lists_ref.shape[0]
    inputs = volts_ref.shape[0]
    count = FR - LATE
    skip = (LATE - 3) * FFT
    loads = [
        pltpu.make_async_copy(lists_hbm, lists_ref, in_sems.at[0]),
        *gain_loads(gains_hbm, gains_ref, in_sems.at[pl.ds(1, 2)]),
        pltpu.make_async_copy(window_hbm, window_ref, in_sems.at[3]),
    ]
    for f in reversed(range(count + 3)):
        cut = slice(f * FFT, (f + 1) * FFT)
        from_cut = slice(skip + f * FFT, skip + (f + 1) * FFT)
        loads.append(
            pltpu.make_async_copy(
                volts_hbm.at[:, from_cut], volts_ref.at[:, cut], in_sems.at[4 + f]
            )
        )
    for load in loads:
        load.start()
    loads[0].wait()

    tail = pltpu.make_async_copy(
        volts_ref.at[:, count * FFT : (count + 3) * FFT], tail_hbm, tail_sem
    )

    def ready():
        for load in loads[1:]:
            load.wait()
        tail.start()

    live_tables(
        lists_ref, channel_ref, table_ref, sign_ref, half_ref, gains_ref, gain_ref, ready
    )

    def read(f, row, lane):
        return volts_ref[pl.ds(row, 16), pl.ds(lane + f * FFT, 128)]

    fir(read, window_ref, weighted_ref, count, inputs)
    width = count * inputs
    store, finish = sender(out_ref, out_hbm, out_sem)
    spectra_and_gains(table_ref, weighted_ref, gain_ref, sign_ref, groups, width, store)
    tail.wait()
    finish()


def late_kernel(
    table_hbm, gain_hbm, sign_hbm, before_hbm, window_hbm, volts_hbm, out_hbm,
    table_ref, gain_ref, sign_ref, before_ref, window_ref, volts_ref, out_ref, weighted_ref, in_sems, out_sem,
):
    groups = out_ref.shape[0]
    inputs = volts_ref.shape[0]
    loads = [
        pltpu.make_async_copy(window_hbm, window_ref, in_sems.at[0]),
        pltpu.make_async_copy(volts_hbm.at[:, 0 : LATE * FFT], volts_ref, in_sems.at[1]),
        pltpu.make_async_copy(before_hbm, before_ref, in_sems.at[2]),
        pltpu.make_async_copy(table_hbm, table_ref, in_sems.at[3]),
        pltpu.make_async_copy(gain_hbm, gain_ref, in_sems.at[4]),
        pltpu.make_async_copy(sign_hbm, sign_ref, in_sems.at[5]),
    ]
    for load in loads:
        load.start()
    for load in loads[:3]:
        load.wait()

    def read(f, row, lane):
        if f < 3:
            return before_ref[pl.ds(row, 16), pl.ds(lane + f * FFT, 128)]
        return volts_ref[pl.ds(row, 16), pl.ds(lane + (f - 3) * FFT, 128)]

    fir(read, window_ref, weighted_ref, LATE, inputs)
    for load in loads[3:]:
        load.wait()
    width = LATE * inputs
    store, finish = sender(out_ref, out_hbm, out_sem)
    spectra_and_gains(table_ref, weighted_ref, gain_ref, sign_ref, groups, width, store)
    finish()


def arrange(received_ref, spread_ref):
    groups, rows, width = received_ref.shape
    low = lax.broadcasted_iota(jnp.int32, (rows, 128), 1) < 64

    def move(pair, carry):
        at = pl.ds(pl.multiple_of(pair * 128, 128), 128)
        for two in range(width // 128):
            cut = slice(two * 128, two * 128 + 128)
            first = received_ref[2 * pair, :, cut].astype(F32)
            second = received_ref[2 * pair + 1, :, cut].astype(F32)
            one = jnp.where(low, first, pltpu.roll(second, 64, 1))
            other = jnp.where(low, pltpu.roll(first, 64, 1), second)
            spread_ref[2 * two * rows : (2 * two + 1) * rows, at] = one.astype(BF16)
            spread_ref[(2 * two + 1) * rows : (2 * two + 2) * rows, at] = other.astype(BF16)
        return carry

    lax.fori_loop(0, groups // 2, move, 0)


def beam_powers(spread_ref, load, weights_ref, step, rows):
    load(step, 0).wait()
    load(step, 1).wait()
    span = pl.ds(pl.multiple_of(step * SPAN, SPAN), SPAN)
    by_real = lax.dot_general(
        spread_ref[...], weights_ref[0, span, :], NT, preferred_element_type=F32
    )
    by_imag = lax.dot_general(
        spread_ref[...], weights_ref[1, span, :], NT, preferred_element_type=F32
    )
    half = rows // 2
    total = None
    for k in range(spread_ref.shape[0] // rows):
        top, middle, end = k * rows, k * rows + half, (k + 1) * rows
        real = by_real[top:middle] - by_imag[middle:end]
        imag = by_real[middle:end] + by_imag[top:middle]
        power = real * real + imag * imag
        total = power if total is None else total + power
    return total


SPAN = 256
BLOCK = 512


def weight_load(weights_hbm, weights_ref, sems, step, part):
    rows = pl.ds(pl.multiple_of(step * SPAN, SPAN), SPAN)
    return pltpu.make_async_copy(
        weights_hbm.at[part, rows, :], weights_ref.at[part, rows, :], sems.at[step, part]
    )


def first_beams_kernel(received_ref, weights_hbm, out_ref, weights_ref, spread_ref, sems):
    steps = BEAMS // SPAN
    for step in range(steps):
        for part in range(2):
            weight_load(weights_hbm, weights_ref, sems, step, part).start()
    arrange(received_ref, spread_ref)
    rows = received_ref.shape[1]

    def tile(step, carry):
        lane = pl.multiple_of(step * SPAN, SPAN)
        load = functools.partial(weight_load, weights_hbm, weights_ref, sems)
        out_ref[:, pl.ds(lane, SPAN)] = beam_powers(spread_ref, load, weights_ref, step, rows)
        return carry

    lax.fori_loop(0, steps, tile, 0)


def arrange_pair(received_ref, near_ref, far_ref):
    groups, rows, width = received_ref.shape
    share = rows // 2
    low = lax.broadcasted_iota(jnp.int32, (rows, 128), 1) < 64

    def move(pair, carry):
        at = pl.ds(pl.multiple_of(pair * 128, 128), 128)
        for two in range(width // 128):
            cut = slice(two * 128, two * 128 + 128)
            first = received_ref[2 * pair, :, cut].astype(F32)
            second = received_ref[2 * pair + 1, :, cut].astype(F32)
            one = jnp.where(low, first, pltpu.roll(second, 64, 1))
            other = jnp.where(low, pltpu.roll(first, 64, 1), second)
            for k, value in ((2 * two, one), (2 * two + 1, other)):
                real, imag = value[:share], value[share:]
                pad = jnp.zeros((32 - share, 128), F32)
                near = jnp.concatenate([real, pad, imag, pad], axis=0)
                far = jnp.concatenate([-imag, pad, real, pad], axis=0)
                near_ref[64 * k : 64 * k + 64, at] = near.astype(BF16)
                far_ref[64 * k : 64 * k + 64, at] = far.astype(BF16)
        return carry

    lax.fori_loop(0, groups // 2, move, 0)


def last_beams_kernel(
    received_ref, weights_hbm, partial_ref, order_ref, out_ref,
    weights_ref, near_ref, far_ref, total_ref, moved_ref, sems,
):
    tiles, rows = moved_ref.shape[:2]
    steps = BEAMS // BLOCK
    here = BLOCK // 128
    for step in range(BEAMS // SPAN):
        for part in range(2):
            weight_load(weights_hbm, weights_ref, sems, step, part).start()
    arrange_pair(received_ref, near_ref, far_ref)

    def powers_of(step):
        at = pl.multiple_of(step * BLOCK, BLOCK)
        powers = []
        for j in range(here):
            turned = total_ref[j * 128 : (j + 1) * 128].T
            power = partial_ref[:, pl.ds(at + j * 128, 128)]
            for part in range(4):
                power = power + turned[part * 32 : part * 32 + rows]
            powers.append(power * np.float32(1.0 / FR))
        for d in range(tiles):
            order = jnp.broadcast_to(order_ref[d : d + 1, :], (rows, 128))
            lane = order & 127
            source = order >> 7
            moved = moved_ref[d]
            for j in range(here):
                moved = jnp.where(
                    source == step * here + j,
                    jnp.take_along_axis(powers[j], lane, axis=1),
                    moved,
                )
            moved_ref[d] = moved

    def tile(step, carry):
        powers_of(lax.rem(step + steps - 1, steps))
        beams = None
        for piece in range(BLOCK // SPAN):
            for part in range(2):
                span = step * (BLOCK // SPAN) + piece
                weight_load(weights_hbm, weights_ref, sems, span, part).wait()
        at = pl.ds(pl.multiple_of(step * BLOCK, BLOCK), BLOCK)
        for part, block_ref in ((0, near_ref), (1, far_ref)):
            product = lax.dot_general(
                weights_ref[part, at, :], block_ref[...], NT, preferred_element_type=F32
            )
            beams = product if beams is None else beams + product
        squares = beams * beams
        total = squares[:, 0:128]
        for j in range(1, beams.shape[1] // 128):
            total = total + squares[:, j * 128 : (j + 1) * 128]
        total_ref[...] = total
        return carry

    total_ref[...] = jnp.zeros_like(total_ref)
    moved_ref[...] = jnp.zeros_like(moved_ref)
    lax.fori_loop(0, steps, tile, 0)
    powers_of(steps - 1)
    low = lax.broadcasted_iota(jnp.int32, (rows, 128), 1) < 64

    def split(d, carry):
        moved = moved_ref[d]
        high = moved.astype(BF16).astype(F32)
        rest = moved - high
        out_ref[2 * d] = jnp.where(low, high, pltpu.roll(rest, 64, 1)).astype(BF16)
        out_ref[2 * d + 1] = jnp.where(low, pltpu.roll(high, 64, 1), rest).astype(BF16)
        return carry

    lax.fori_loop(0, tiles, split, 0, unroll=4)


def middle_kernel(
    lists_hbm, gains_hbm, filter_hbm, table_hbm, gain_hbm, sign_hbm, high_hbm, low_hbm,
    table_ref, gain_ref, sign_ref, lists_ref, gains_ref, channel_ref, half_ref, pick_ref, filter_ref, high_ref, low_ref, sems,
):
    loads = [
        pltpu.make_async_copy(lists_hbm, lists_ref, sems.at[0]),
        pltpu.make_async_copy(filter_hbm, filter_ref, sems.at[2]),
        *gain_loads(gains_hbm, gains_ref, sems.at[pl.ds(8, 2)]),
    ]
    for load in loads:
        load.start()
    loads[0].wait()

    def ready():
        for load in loads[2:]:
            load.wait()

    live_tables(
        lists_ref, channel_ref, table_ref, sign_ref, half_ref, gains_ref, gain_ref, ready, pick_ref
    )
    saves = [
        pltpu.make_async_copy(table_ref, table_hbm, sems.at[3]),
        pltpu.make_async_copy(gain_ref, gain_hbm, sems.at[4]),
        pltpu.make_async_copy(sign_ref, sign_hbm, sems.at[5]),
    ]
    for save in saves:
        save.start()
    loads[1].wait()

    def columns(step, carry):
        at = pl.ds(pl.multiple_of(step * 256, 256), 256)
        whole = filter_ref[:, at]
        high = whole.astype(BF16)
        low = (whole - high.astype(F32)).astype(BF16)
        high_ref[:, at] = jnp.dot(pick_ref[...], high, preferred_element_type=F32).astype(BF16)
        low_ref[:, at] = jnp.dot(pick_ref[...], low, preferred_element_type=F32).astype(BF16)
        return carry

    lax.fori_loop(0, CHANNELS // 256, columns, 0)
    saves = saves + [
        pltpu.make_async_copy(high_ref, high_hbm, sems.at[6]),
        pltpu.make_async_copy(low_ref, low_hbm, sems.at[7]),
    ]
    for save in saves[3:]:
        save.start()
    for save in saves:
        save.wait()


def filter_kernel(powers_ref, high_ref, low_ref, out_ref):
    powers = powers_ref[...]
    both = lax.dot_general(powers, high_ref[...], TN, preferred_element_type=F32)
    rest = lax.dot_general(powers, low_ref[...], TN, preferred_element_type=F32)
    half = out_ref.shape[0]
    out_ref[...] = (both[half:] + rest[:half]) + both[:half]


def cost(flops, data=0):
    return pl.CostEstimate(flops=int(flops), bytes_accessed=int(data), transcendentals=0)


def params(limit=None, **more):
    return pltpu.CompilerParams(vmem_limit_bytes=limit, **more)


WHOLE = 67043328
MOST = WHOLE - (12 << 20)
SOME = WHOLE - (25 << 16)
VM = pl.BlockSpec(memory_space=pltpu.VMEM)
HBM = pl.BlockSpec(memory_space=pltpu.MemorySpace.HBM)


def exchange(block):
    return lax.all_to_all(block, "feed", split_axis=0, concat_axis=0, tiled=True)


def stages(voltages, gains, beam_weights, delay_filter, channel_lists, beam_order):
    groups = lax.axis_size("feed")
    blocks = lax.axis_size("tm")
    inputs = voltages.shape[0]
    share = LIVE // groups
    mine = BEAMS // groups
    every = groups * inputs
    window = jnp.asarray(make_window(FFT))
    count = FR - LATE
    early = count * inputs
    late = LATE * inputs
    mib = 1 << 20
    kept = (
        jax.ShapeDtypeStruct((2 * LIVE, FFT // 2), BF16),
        jax.ShapeDtypeStruct((LIVE, 256), F32),
        jax.ShapeDtypeStruct((LIVE, 128), F32),
    )
    scratch = tuple(pltpu.VMEM(k.shape, k.dtype) for k in kept)
    gains = gains.reshape(2 * inputs, CHANNELS)
    spectra, tail = pl.pallas_call(
        early_kernel,
        out_shape=(
            jax.ShapeDtypeStruct((groups, 2 * share, early), BF16),
            jax.ShapeDtypeStruct((inputs, 3 * FFT), BF16),
        ),
        in_specs=[HBM] * 4,
        out_specs=(HBM,) * 2,
        scratch_shapes=[
            pltpu.VMEM(channel_lists.shape, jnp.int32),
            pltpu.VMEM((4 * inputs, CHANNELS // 2), BF16),
            pltpu.VMEM(window.shape, F32),
            pltpu.VMEM((inputs, (count + 3) * FFT), BF16),
            pltpu.VMEM((groups, 2 * share, early), BF16),
            *scratch,
            pltpu.VMEM((LIVE, CHANNELS // 2), BF16),
            pltpu.VMEM((LIVE, 128), jnp.int32),
            pltpu.VMEM((early, FFT), BF16),
            pltpu.SemaphoreType.DMA((count + 7,)),
            pltpu.SemaphoreType.DMA,
            pltpu.SemaphoreType.DMA,
        ],
        compiler_params=params(WHOLE),
        cost_estimate=cost(2 * 2 * LIVE * FFT * early),
        name="early",
    )(channel_lists, gains, window, voltages)
    before = lax.ppermute(tail, "tm", [(i, i + 1) for i in range(blocks - 1)])
    first = exchange(spectra)
    table, gain, sign, filter_high, filter_low = pl.pallas_call(
        middle_kernel,
        out_shape=(*kept, *(jax.ShapeDtypeStruct((LIVE, CHANNELS), BF16),) * 2),
        in_specs=[HBM] * 3,
        out_specs=(HBM,) * 5,
        scratch_shapes=[
            *scratch,
            pltpu.VMEM(channel_lists.shape, jnp.int32),
            pltpu.VMEM((4 * inputs, CHANNELS // 2), BF16),
            pltpu.VMEM((LIVE, 128), jnp.int32),
            pltpu.VMEM((LIVE, CHANNELS // 2), BF16),
            pltpu.VMEM((LIVE, CHANNELS), BF16),
            pltpu.VMEM((CHANNELS, CHANNELS), F32),
            pltpu.VMEM((LIVE, CHANNELS), BF16),
            pltpu.VMEM((LIVE, CHANNELS), BF16),
            pltpu.SemaphoreType.DMA((10,)),
        ],
        compiler_params=params(SOME),
        cost_estimate=cost(4 * LIVE * CHANNELS * CHANNELS),
        name="middle",
    )(channel_lists, gains, delay_filter)
    spectra = pl.pallas_call(
        late_kernel,
        out_shape=jax.ShapeDtypeStruct((groups, 2 * share, late), BF16),
        in_specs=[HBM] * 6,
        out_specs=HBM,
        scratch_shapes=[
            *scratch,
            pltpu.VMEM(before.shape, BF16),
            pltpu.VMEM(window.shape, F32),
            pltpu.VMEM((inputs, LATE * FFT), BF16),
            pltpu.VMEM((groups, 2 * share, late), BF16),
            pltpu.VMEM((late, FFT), BF16),
            pltpu.SemaphoreType.DMA((6,)),
            pltpu.SemaphoreType.DMA,
        ],
        compiler_params=params(SOME),
        cost_estimate=cost(2 * 2 * LIVE * FFT * late),
        name="late",
    )(table, gain, sign, before, window, voltages)
    second = exchange(spectra)
    partial = pl.pallas_call(
        first_beams_kernel,
        out_shape=jax.ShapeDtypeStruct((share, BEAMS), F32),
        in_specs=[VM, HBM],
        out_specs=VM,
        scratch_shapes=[
            pltpu.VMEM((2, BEAMS, every), BF16),
            pltpu.VMEM((2 * share * count, every), BF16),
            pltpu.SemaphoreType.DMA((BEAMS // SPAN, 2)),
        ],
        compiler_params=params(MOST),
        cost_estimate=cost(2 * 2 * BEAMS * every * 2 * share * count),
        name="first_beams",
    )(first, beam_weights)
    powers = pl.pallas_call(
        last_beams_kernel,
        out_shape=jax.ShapeDtypeStruct((groups, share, 2 * mine), BF16),
        in_specs=[VM, HBM, VM, VM],
        out_specs=VM,
        scratch_shapes=[
            pltpu.VMEM((2, BEAMS, every), BF16),
            pltpu.VMEM((64 * LATE, every), BF16),
            pltpu.VMEM((64 * LATE, every), BF16),
            pltpu.VMEM((BLOCK, 128), F32),
            pltpu.VMEM((BEAMS // 128, share, 128), F32),
            pltpu.SemaphoreType.DMA((BEAMS // SPAN, 2)),
        ],
        compiler_params=params(MOST),
        cost_estimate=cost(2 * 2 * BEAMS * every * 2 * share * LATE),
        name="last_beams",
    )(second, beam_weights, partial, beam_order.reshape(BEAMS // 128, 128))
    owned = exchange(powers)
    filtered = pl.pallas_call(
        filter_kernel,
        out_shape=jax.ShapeDtypeStruct((mine, CHANNELS), F32),
        in_specs=[VM] * 3,
        out_specs=VM,
        compiler_params=params(20 * mib),
        cost_estimate=cost(4 * LIVE * CHANNELS * 2 * mine),
        name="filter",
    )(owned.reshape(LIVE, 2 * mine), filter_high, filter_low)
    return filtered.reshape(1, mine, CHANNELS)


def solution(mesh):
    placed = (P("feed", "tm"), P(None, "feed", None), P(), P(), P(), P())
    return jax.shard_map(
        stages, mesh=mesh, in_specs=placed, out_specs=P("tm", "feed", None), check_vma=False
    )
```

```python
import functools

import jax
import jax.numpy as jnp
import numpy as np
from jax import lax
from jax.experimental import pallas as pl
from jax.experimental.pallas import tpu as pltpu
from jax.sharding import PartitionSpec as P


FFT = 2048
BEAMS = 2048
CHANNELS = 1024
LIVE = 768
FR = 12
LATE = 4
NT = (((1,), (1,)), ((), ()))
TN = (((0,), (0,)), ((), ()))
F32 = jnp.float32
BF16 = jnp.bfloat16


def make_window(length):
    places = np.arange(4 * length, dtype=np.float64)
    centred = (places - 2.0 * length + 0.5) / length
    taper = 0.5 - 0.5 * np.cos(2.0 * np.pi * (places + 0.5) / (4.0 * length))
    return (np.sinc(centred) * taper).reshape(4, length).astype(np.float32)


def cos_sin(phase):
    quarter = lax.shift_right_logical(phase + 256, 9)
    x = (phase - quarter * 512).astype(F32) * np.float32(np.pi / 1024)
    y = x * x
    s = x * (1.0 + y * (-1.0 / 6 + y * (1.0 / 120 + y * (-1.0 / 5040 + y * (1.0 / 362880)))))
    c = 1.0 + y * (
        -0.5 + y * (1.0 / 24 + y * (-1.0 / 720 + y * (1.0 / 40320 + y * (-1.0 / 3628800))))
    )
    odd = (quarter & 1) == 1
    cos = jnp.where(odd, s, c)
    sin = jnp.where(odd, c, s)
    cos = jnp.where(((quarter + 1) & 2) == 2, -cos, cos)
    sin = jnp.where((quarter & 2) == 2, -sin, sin)
    return cos, sin


def slots_of(lists):
    groups, places = lists.shape
    both = 2 * groups
    odd = (lists & 1) == 1
    evens = jnp.where((lists >= 0) & ~odd, 1.0, 0.0)
    odds = jnp.where((lists >= 0) & odd, 1.0, 0.0)
    marks = jnp.concatenate([evens, odds], axis=0)
    ahead = lax.broadcasted_iota(jnp.int32, (places, places), 0)
    place = lax.broadcasted_iota(jnp.int32, (places, places), 1)
    earlier = jnp.where(ahead < place, 1.0, 0.0).astype(BF16)
    rank = jnp.dot(marks.astype(BF16), earlier, preferred_element_type=F32)
    keys = jnp.where(marks > 0.0, rank, -1.0).astype(BF16)
    counts = jnp.sum(marks, axis=1, keepdims=True)
    above = lax.broadcasted_iota(jnp.int32, (both, both), 0)
    here = lax.broadcasted_iota(jnp.int32, (both, both), 1)
    wide = jnp.broadcast_to(counts, (both, both))
    first = jnp.sum(jnp.where(above < here, wide, 0.0), axis=0, keepdims=True)
    count = jnp.sum(jnp.where(above == here, wide, 0.0), axis=0, keepdims=True)
    slot = lax.broadcasted_iota(jnp.int32, (LIVE, both), 0).astype(F32)
    inside = (slot >= first) & (slot < first + count)
    pick = jnp.where(inside, 1.0, 0.0).astype(BF16)
    wanted = jnp.sum(jnp.where(inside, slot - first, 0.0), axis=1, keepdims=True)
    known = jnp.maximum(lists, 0)
    known = jnp.concatenate([known, known], axis=0)
    high = (known >> 5).astype(F32).astype(BF16)
    low = (known & 31).astype(F32).astype(BF16)
    rows = 32.0 * jnp.dot(pick, high, preferred_element_type=F32) + jnp.dot(
        pick, low, preferred_element_type=F32
    )
    key = jnp.dot(pick, keys, preferred_element_type=F32)
    return jnp.sum(jnp.where(key == wanted, rows, 0.0), axis=1, keepdims=True)


def fir(read, window_ref, weighted_ref, count, inputs):
    half = FFT // 2

    def totals(row, lane):
        taps = [window_ref[pl.ds(t, 1), pl.ds(lane, 128)] for t in range(4)]
        frames = [read(f, row, lane).astype(F32) for f in range(count + 3)]
        out = []
        for k in range(count):
            total = taps[0] * frames[k]
            for t in range(1, 4):
                total = total + taps[t] * frames[k + t]
            out.append(total)
        return out

    def tile(step, carry):
        lane = pl.multiple_of(step * 128, 128)
        for row in range(0, inputs, 16):
            near = totals(row, lane)
            far = totals(row, lane + half)
            for k in range(count):
                at = pl.ds(k * inputs + row, 16)
                weighted_ref[at, pl.ds(lane, 128)] = (near[k] + far[k]).astype(BF16)
                weighted_ref[at, pl.ds(lane + half, 128)] = (near[k] - far[k]).astype(BF16)
        return carry

    lax.fori_loop(0, half // 128, tile, 0, unroll=2)


def spectra_and_gains(table_ref, weighted_ref, gain_ref, sign_ref, groups, width, store):
    share = LIVE // groups
    size = 2 * share
    pure = (LIVE - CHANNELS // 2) // share
    half = FFT // 2

    def part(step, carry):
        lane = pl.multiple_of(step * 256, 256)
        evens = lax.dot_general(
            table_ref[0 : (groups - pure) * size, :],
            weighted_ref[pl.ds(lane, 256), 0:half],
            NT,
            preferred_element_type=F32,
        )
        odds = lax.dot_general(
            table_ref[pure * size :, :],
            weighted_ref[pl.ds(lane, 256), half:FFT],
            NT,
            preferred_element_type=F32,
        )
        for g in range(groups):
            own = slice(g * share, (g + 1) * share)
            real_gain = gain_ref[own, 0:128]
            imag_gain = gain_ref[own, 128:256]
            even = sign_ref[own, :] > 0.0
            for piece in range(2):
                cut = slice(piece * 128, piece * 128 + 128)
                if g < groups - pure:
                    real = evens[g * size : g * size + share, cut]
                    imag = evens[g * size + share : (g + 1) * size, cut]
                if g >= pure:
                    at = (g - pure) * size
                    odd_real = odds[at : at + share, cut]
                    odd_imag = odds[at + share : at + size, cut]
                    if g < groups - pure:
                        real = jnp.where(even, real, odd_real)
                        imag = jnp.where(even, imag, odd_imag)
                    else:
                        real, imag = odd_real, odd_imag
                both = jnp.concatenate(
                    [
                        real * real_gain - imag * imag_gain,
                        real * imag_gain + imag * real_gain,
                    ],
                    axis=0,
                )
                store(g, lane + piece * 128, both.astype(BF16))
            if (g + 1) % SENT == 0:
                store(g, lane, None)
        return carry

    lax.fori_loop(0, width // 256, part, 0)


SENT = 4


def sender(out_vmem, out_hbm, sem):

    def copy(g, lane):
        at = (slice(g + 1 - SENT, g + 1), slice(None), pl.ds(lane, 256))
        return pltpu.make_async_copy(out_vmem.at[at], out_hbm.at[at], sem)

    def store(g, lane, value):
        if value is None:
            copy(g, lane).start()
        else:
            out_vmem[g, :, pl.ds(lane, 128)] = value

    def finish():
        pltpu.make_async_copy(out_vmem, out_hbm, sem).wait()

    return store, finish


def gain_loads(gains_hbm, gains_ref, sems):
    rows, half = gains_hbm.shape[0], CHANNELS // 2
    return [
        pltpu.make_async_copy(
            gains_hbm.at[:, part * half : (part + 1) * half],
            gains_ref.at[part * rows : (part + 1) * rows, :],
            sems.at[part],
        )
        for part in range(2)
    ]


def live_tables(
    lists_ref, channel_ref, table_ref, sign_ref, half_ref, gains_ref, gain_ref, ready, pick_ref=None
):
    groups = lists_ref.shape[0]
    share = LIVE // groups
    channel_ref[...] = jnp.broadcast_to(slots_of(lists_ref[...]), (LIVE, 128)).astype(jnp.int32)

    def table_rows(pair, carry):
        at = pl.multiple_of(pair * 2 * share, 2 * share)
        channel = channel_ref[pl.ds(at, 2 * share), :]
        lane = lax.broadcasted_iota(jnp.int32, channel.shape, 1)
        cos, sin = cos_sin((channel * lane) & (FFT - 1))
        scale = np.float32(FFT ** (-0.5))
        real, imag = cos * scale, -sin * scale
        half_cos = jnp.broadcast_to(cos[:, 64:65], cos.shape)
        half_sin = jnp.broadcast_to(sin[:, 64:65], sin.shape)
        turn_cos = 2.0 * half_cos * half_cos - 1.0
        turn_sin = 2.0 * half_cos * half_sin
        twice = 2.0 * turn_cos
        last = None
        row = pl.multiple_of(pair * 4 * share, 4 * share)
        for j in range(FFT // 256):
            both = jnp.concatenate(
                [real[:share], imag[:share], real[share:], imag[share:]], axis=0
            )
            table_ref[pl.ds(row, 4 * share), j * 128 : (j + 1) * 128] = both.astype(BF16)
            if last is None:
                following = (
                    real * turn_cos + imag * turn_sin,
                    imag * turn_cos - real * turn_sin,
                )
            else:
                following = (twice * real - last[0], twice * imag - last[1])
            last = (real, imag)
            real, imag = following
        sign_ref[pl.ds(at, 2 * share), :] = jnp.where((channel & 1) == 1, -1.0, 1.0)
        lower = channel & (CHANNELS // 2 - 1)
        picks = [(half_ref, lower, CHANNELS // 2)]
        if pick_ref is not None:
            picks.append((pick_ref, channel, CHANNELS))
        for ref, wanted, width in picks:
            for j in range(width // 128):
                ref[pl.ds(at, 2 * share), j * 128 : (j + 1) * 128] = jnp.where(
                    wanted == lane + j * 128, 1.0, 0.0
                ).astype(BF16)
        return carry

    lax.fori_loop(0, groups // 2, table_rows, 0, unroll=4)
    ready()
    either = lax.dot_general(half_ref[...], gains_ref[...], NT, preferred_element_type=F32)
    upper = channel_ref[...] >= CHANNELS // 2
    gain = jnp.where(upper, either[:, 128:256], either[:, 0:128])
    turned = pltpu.roll(gain, 64, 1)
    low = lax.broadcasted_iota(jnp.int32, gain.shape, 1) < 64
    gain_ref[:, 0:128] = jnp.where(low, gain, turned)
    gain_ref[:, 128:256] = jnp.where(low, turned, gain)


def early_kernel(
    lists_hbm, gains_hbm, window_hbm, volts_hbm, out_hbm, tail_hbm,
    lists_ref, gains_ref, window_ref, volts_ref, out_ref, table_ref, gain_ref, sign_ref, half_ref,
    channel_ref, weighted_ref, in_sems, out_sem, tail_sem,
):
    groups = lists_ref.shape[0]
    inputs = volts_ref.shape[0]
    count = FR - LATE
    skip = (LATE - 3) * FFT
    loads = [
        pltpu.make_async_copy(lists_hbm, lists_ref, in_sems.at[0]),
        *gain_loads(gains_hbm, gains_ref, in_sems.at[pl.ds(1, 2)]),
        pltpu.make_async_copy(window_hbm, window_ref, in_sems.at[3]),
    ]
    for f in reversed(range(count + 3)):
        cut = slice(f * FFT, (f + 1) * FFT)
        from_cut = slice(skip + f * FFT, skip + (f + 1) * FFT)
        loads.append(
            pltpu.make_async_copy(
                volts_hbm.at[:, from_cut], volts_ref.at[:, cut], in_sems.at[4 + f]
            )
        )
    for load in loads:
        load.start()
    loads[0].wait()

    tail = pltpu.make_async_copy(
        volts_ref.at[:, count * FFT : (count + 3) * FFT], tail_hbm, tail_sem
    )

    def ready():
        for load in loads[1:]:
            load.wait()
        tail.start()

    live_tables(
        lists_ref, channel_ref, table_ref, sign_ref, half_ref, gains_ref, gain_ref, ready
    )

    def read(f, row, lane):
        return volts_ref[pl.ds(row, 16), pl.ds(lane + f * FFT, 128)]

    fir(read, window_ref, weighted_ref, count, inputs)
    width = count * inputs
    store, finish = sender(out_ref, out_hbm, out_sem)
    spectra_and_gains(table_ref, weighted_ref, gain_ref, sign_ref, groups, width, store)
    tail.wait()
    finish()


def late_kernel(
    table_hbm, gain_hbm, sign_hbm, before_hbm, window_hbm, volts_hbm, out_hbm,
    table_ref, gain_ref, sign_ref, before_ref, window_ref, volts_ref, out_ref, weighted_ref, in_sems, out_sem,
):
    groups = out_ref.shape[0]
    inputs = volts_ref.shape[0]
    loads = [
        pltpu.make_async_copy(window_hbm, window_ref, in_sems.at[0]),
        pltpu.make_async_copy(volts_hbm.at[:, 0 : LATE * FFT], volts_ref, in_sems.at[1]),
        pltpu.make_async_copy(before_hbm, before_ref, in_sems.at[2]),
        pltpu.make_async_copy(table_hbm, table_ref, in_sems.at[3]),
        pltpu.make_async_copy(gain_hbm, gain_ref, in_sems.at[4]),
        pltpu.make_async_copy(sign_hbm, sign_ref, in_sems.at[5]),
    ]
    for load in loads:
        load.start()
    for load in loads[:3]:
        load.wait()

    def read(f, row, lane):
        if f < 3:
            return before_ref[pl.ds(row, 16), pl.ds(lane + f * FFT, 128)]
        return volts_ref[pl.ds(row, 16), pl.ds(lane + (f - 3) * FFT, 128)]

    fir(read, window_ref, weighted_ref, LATE, inputs)
    for load in loads[3:]:
        load.wait()
    width = LATE * inputs
    store, finish = sender(out_ref, out_hbm, out_sem)
    spectra_and_gains(table_ref, weighted_ref, gain_ref, sign_ref, groups, width, store)
    finish()


def arrange(received_ref, spread_ref):
    groups, rows, width = received_ref.shape
    low = lax.broadcasted_iota(jnp.int32, (rows, 128), 1) < 64

    def move(pair, carry):
        at = pl.ds(pl.multiple_of(pair * 128, 128), 128)
        for two in range(width // 128):
            cut = slice(two * 128, two * 128 + 128)
            first = received_ref[2 * pair, :, cut].astype(F32)
            second = received_ref[2 * pair + 1, :, cut].astype(F32)
            one = jnp.where(low, first, pltpu.roll(second, 64, 1))
            other = jnp.where(low, pltpu.roll(first, 64, 1), second)
            spread_ref[2 * two * rows : (2 * two + 1) * rows, at] = one.astype(BF16)
            spread_ref[(2 * two + 1) * rows : (2 * two + 2) * rows, at] = other.astype(BF16)
        return carry

    lax.fori_loop(0, groups // 2, move, 0, unroll=2)


def beam_powers(spread_ref, load, weights_ref, step, rows):
    load(step, 0).wait()
    load(step, 1).wait()
    span = pl.ds(pl.multiple_of(step * SPAN, SPAN), SPAN)
    by_real = lax.dot_general(
        spread_ref[...], weights_ref[0, span, :], NT, preferred_element_type=F32
    )
    by_imag = lax.dot_general(
        spread_ref[...], weights_ref[1, span, :], NT, preferred_element_type=F32
    )
    half = rows // 2
    total = None
    for k in range(spread_ref.shape[0] // rows):
        top, middle, end = k * rows, k * rows + half, (k + 1) * rows
        real = by_real[top:middle] - by_imag[middle:end]
        imag = by_real[middle:end] + by_imag[top:middle]
        power = real * real + imag * imag
        total = power if total is None else total + power
    return total


SPAN = 256
BLOCK = 512


def weight_load(weights_hbm, weights_ref, sems, step, part):
    rows = pl.ds(pl.multiple_of(step * SPAN, SPAN), SPAN)
    return pltpu.make_async_copy(
        weights_hbm.at[part, rows, :], weights_ref.at[part, rows, :], sems.at[step, part]
    )


def first_beams_kernel(received_ref, weights_hbm, out_ref, weights_ref, spread_ref, sems):
    steps = BEAMS // SPAN
    for step in range(steps):
        for part in range(2):
            weight_load(weights_hbm, weights_ref, sems, step, part).start()
    arrange(received_ref, spread_ref)
    rows = received_ref.shape[1]

    def tile(step, carry):
        lane = pl.multiple_of(step * SPAN, SPAN)
        load = functools.partial(weight_load, weights_hbm, weights_ref, sems)
        out_ref[:, pl.ds(lane, SPAN)] = beam_powers(spread_ref, load, weights_ref, step, rows)
        return carry

    lax.fori_loop(0, steps, tile, 0)


def arrange_pair(received_ref, near_ref, far_ref):
    groups, rows, width = received_ref.shape
    share = rows // 2
    low = lax.broadcasted_iota(jnp.int32, (rows, 128), 1) < 64

    def move(pair, carry):
        at = pl.ds(pl.multiple_of(pair * 128, 128), 128)
        for two in range(width // 128):
            cut = slice(two * 128, two * 128 + 128)
            first = received_ref[2 * pair, :, cut].astype(F32)
            second = received_ref[2 * pair + 1, :, cut].astype(F32)
            one = jnp.where(low, first, pltpu.roll(second, 64, 1))
            other = jnp.where(low, pltpu.roll(first, 64, 1), second)
            for k, value in ((2 * two, one), (2 * two + 1, other)):
                real, imag = value[:share], value[share:]
                pad = jnp.zeros((32 - share, 128), F32)
                near = jnp.concatenate([real, pad, imag, pad], axis=0)
                far = jnp.concatenate([-imag, pad, real, pad], axis=0)
                near_ref[64 * k : 64 * k + 64, at] = near.astype(BF16)
                far_ref[64 * k : 64 * k + 64, at] = far.astype(BF16)
        return carry

    lax.fori_loop(0, groups // 2, move, 0, unroll=2)


def last_beams_kernel(
    received_ref, weights_hbm, partial_ref, order_ref, out_ref,
    weights_ref, near_ref, far_ref, total_ref, moved_ref, sems,
):
    tiles, rows = moved_ref.shape[:2]
    steps = BEAMS // BLOCK
    here = BLOCK // 128
    for step in range(BEAMS // SPAN):
        for part in range(2):
            weight_load(weights_hbm, weights_ref, sems, step, part).start()
    arrange_pair(received_ref, near_ref, far_ref)

    def powers_of(step):
        at = pl.multiple_of(step * BLOCK, BLOCK)
        powers = []
        for j in range(here):
            turned = total_ref[j * 128 : (j + 1) * 128].T
            power = partial_ref[:, pl.ds(at + j * 128, 128)]
            for part in range(4):
                power = power + turned[part * 32 : part * 32 + rows]
            powers.append(power * np.float32(1.0 / FR))
        for d in range(tiles):
            order = jnp.broadcast_to(order_ref[d : d + 1, :], (rows, 128))
            lane = order & 127
            source = order >> 7
            moved = moved_ref[d]
            for j in range(here):
                moved = jnp.where(
                    source == step * here + j,
                    jnp.take_along_axis(powers[j], lane, axis=1),
                    moved,
                )
            moved_ref[d] = moved

    def tile(step, carry):
        powers_of(lax.rem(step + steps - 1, steps))
        beams = None
        for piece in range(BLOCK // SPAN):
            for part in range(2):
                span = step * (BLOCK // SPAN) + piece
                weight_load(weights_hbm, weights_ref, sems, span, part).wait()
        at = pl.ds(pl.multiple_of(step * BLOCK, BLOCK), BLOCK)
        for part, block_ref in ((0, near_ref), (1, far_ref)):
            product = lax.dot_general(
                weights_ref[part, at, :], block_ref[...], NT, preferred_element_type=F32
            )
            beams = product if beams is None else beams + product
        squares = beams * beams
        total = squares[:, 0:128]
        for j in range(1, beams.shape[1] // 128):
            total = total + squares[:, j * 128 : (j + 1) * 128]
        total_ref[...] = total
        return carry

    total_ref[...] = jnp.zeros_like(total_ref)
    moved_ref[...] = jnp.zeros_like(moved_ref)
    lax.fori_loop(0, steps, tile, 0)
    powers_of(steps - 1)
    low = lax.broadcasted_iota(jnp.int32, (rows, 128), 1) < 64

    def split(d, carry):
        moved = moved_ref[d]
        high = moved.astype(BF16).astype(F32)
        rest = moved - high
        out_ref[2 * d] = jnp.where(low, high, pltpu.roll(rest, 64, 1)).astype(BF16)
        out_ref[2 * d + 1] = jnp.where(low, pltpu.roll(high, 64, 1), rest).astype(BF16)
        return carry

    lax.fori_loop(0, tiles, split, 0, unroll=4)


def middle_kernel(
    lists_hbm, gains_hbm, filter_hbm, table_hbm, gain_hbm, sign_hbm, high_hbm, low_hbm,
    table_ref, gain_ref, sign_ref, lists_ref, gains_ref, channel_ref, half_ref, pick_ref, filter_ref, high_ref, low_ref, sems,
):
    loads = [
        pltpu.make_async_copy(lists_hbm, lists_ref, sems.at[0]),
        pltpu.make_async_copy(filter_hbm, filter_ref, sems.at[2]),
        *gain_loads(gains_hbm, gains_ref, sems.at[pl.ds(8, 2)]),
    ]
    for load in loads:
        load.start()
    loads[0].wait()

    def ready():
        for load in loads[2:]:
            load.wait()

    live_tables(
        lists_ref, channel_ref, table_ref, sign_ref, half_ref, gains_ref, gain_ref, ready, pick_ref
    )
    saves = [
        pltpu.make_async_copy(table_ref, table_hbm, sems.at[3]),
        pltpu.make_async_copy(gain_ref, gain_hbm, sems.at[4]),
        pltpu.make_async_copy(sign_ref, sign_hbm, sems.at[5]),
    ]
    for save in saves:
        save.start()
    loads[1].wait()

    def columns(step, carry):
        at = pl.ds(pl.multiple_of(step * 256, 256), 256)
        whole = filter_ref[:, at]
        high = whole.astype(BF16)
        low = (whole - high.astype(F32)).astype(BF16)
        high_ref[:, at] = jnp.dot(pick_ref[...], high, preferred_element_type=F32).astype(BF16)
        low_ref[:, at] = jnp.dot(pick_ref[...], low, preferred_element_type=F32).astype(BF16)
        return carry

    lax.fori_loop(0, CHANNELS // 256, columns, 0)
    saves = saves + [
        pltpu.make_async_copy(high_ref, high_hbm, sems.at[6]),
        pltpu.make_async_copy(low_ref, low_hbm, sems.at[7]),
    ]
    for save in saves[3:]:
        save.start()
    for save in saves:
        save.wait()


def filter_kernel(powers_ref, high_ref, low_ref, out_hbm, out_ref, sems):
    half = out_ref.shape[0]
    copies = []
    for n in range(2):
        cut = slice(n * CHANNELS // 2, (n + 1) * CHANNELS // 2)
        powers = powers_ref[...]
        both = lax.dot_general(powers, high_ref[:, cut], TN, preferred_element_type=F32)
        rest = lax.dot_general(powers, low_ref[:, cut], TN, preferred_element_type=F32)
        out_ref[:, cut] = (both[half:] + rest[:half]) + both[:half]
        copies.append(
            pltpu.make_async_copy(out_ref.at[:, cut], out_hbm.at[:, cut], sems.at[n])
        )
        copies[-1].start()
    for copy in copies:
        copy.wait()


def cost(flops, data=0):
    return pl.CostEstimate(flops=int(flops), bytes_accessed=int(data), transcendentals=0)


def params(limit=None, **more):
    return pltpu.CompilerParams(vmem_limit_bytes=limit, **more)


WHOLE = 67043328
MOST = WHOLE - (12 << 20)
SOME = WHOLE - (25 << 16)
VM = pl.BlockSpec(memory_space=pltpu.VMEM)
HBM = pl.BlockSpec(memory_space=pltpu.MemorySpace.HBM)


def exchange(block):
    return lax.all_to_all(block, "feed", split_axis=0, concat_axis=0, tiled=True)


def stages(voltages, gains, beam_weights, delay_filter, channel_lists, beam_order):
    groups = lax.axis_size("feed")
    blocks = lax.axis_size("tm")
    inputs = voltages.shape[0]
    share = LIVE // groups
    mine = BEAMS // groups
    every = groups * inputs
    window = jnp.asarray(make_window(FFT))
    count = FR - LATE
    early = count * inputs
    late = LATE * inputs
    mib = 1 << 20
    kept = (
        jax.ShapeDtypeStruct((2 * LIVE, FFT // 2), BF16),
        jax.ShapeDtypeStruct((LIVE, 256), F32),
        jax.ShapeDtypeStruct((LIVE, 128), F32),
    )
    scratch = tuple(pltpu.VMEM(k.shape, k.dtype) for k in kept)
    gains = gains.reshape(2 * inputs, CHANNELS)
    spectra, tail = pl.pallas_call(
        early_kernel,
        out_shape=(
            jax.ShapeDtypeStruct((groups, 2 * share, early), BF16),
            jax.ShapeDtypeStruct((inputs, 3 * FFT), BF16),
        ),
        in_specs=[HBM] * 4,
        out_specs=(HBM,) * 2,
        scratch_shapes=[
            pltpu.VMEM(channel_lists.shape, jnp.int32),
            pltpu.VMEM((4 * inputs, CHANNELS // 2), BF16),
            pltpu.VMEM(window.shape, F32),
            pltpu.VMEM((inputs, (count + 3) * FFT), BF16),
            pltpu.VMEM((groups, 2 * share, early), BF16),
            *scratch,
            pltpu.VMEM((LIVE, CHANNELS // 2), BF16),
            pltpu.VMEM((LIVE, 128), jnp.int32),
            pltpu.VMEM((early, FFT), BF16),
            pltpu.SemaphoreType.DMA((count + 7,)),
            pltpu.SemaphoreType.DMA,
            pltpu.SemaphoreType.DMA,
        ],
        compiler_params=params(WHOLE),
        cost_estimate=cost(2 * 2 * LIVE * FFT * early),
        name="early",
    )(channel_lists, gains, window, voltages)
    before = lax.ppermute(tail, "tm", [(i, i + 1) for i in range(blocks - 1)])
    first = exchange(spectra)
    table, gain, sign, filter_high, filter_low = pl.pallas_call(
        middle_kernel,
        out_shape=(*kept, *(jax.ShapeDtypeStruct((LIVE, CHANNELS), BF16),) * 2),
        in_specs=[HBM] * 3,
        out_specs=(HBM,) * 5,
        scratch_shapes=[
            *scratch,
            pltpu.VMEM(channel_lists.shape, jnp.int32),
            pltpu.VMEM((4 * inputs, CHANNELS // 2), BF16),
            pltpu.VMEM((LIVE, 128), jnp.int32),
            pltpu.VMEM((LIVE, CHANNELS // 2), BF16),
            pltpu.VMEM((LIVE, CHANNELS), BF16),
            pltpu.VMEM((CHANNELS, CHANNELS), F32),
            pltpu.VMEM((LIVE, CHANNELS), BF16),
            pltpu.VMEM((LIVE, CHANNELS), BF16),
            pltpu.SemaphoreType.DMA((10,)),
        ],
        compiler_params=params(SOME),
        cost_estimate=cost(4 * LIVE * CHANNELS * CHANNELS),
        name="middle",
    )(channel_lists, gains, delay_filter)
    spectra = pl.pallas_call(
        late_kernel,
        out_shape=jax.ShapeDtypeStruct((groups, 2 * share, late), BF16),
        in_specs=[HBM] * 6,
        out_specs=HBM,
        scratch_shapes=[
            *scratch,
            pltpu.VMEM(before.shape, BF16),
            pltpu.VMEM(window.shape, F32),
            pltpu.VMEM((inputs, LATE * FFT), BF16),
            pltpu.VMEM((groups, 2 * share, late), BF16),
            pltpu.VMEM((late, FFT), BF16),
            pltpu.SemaphoreType.DMA((6,)),
            pltpu.SemaphoreType.DMA,
        ],
        compiler_params=params(SOME),
        cost_estimate=cost(2 * 2 * LIVE * FFT * late),
        name="late",
    )(table, gain, sign, before, window, voltages)
    second = exchange(spectra)
    partial = pl.pallas_call(
        first_beams_kernel,
        out_shape=jax.ShapeDtypeStruct((share, BEAMS), F32),
        in_specs=[VM, HBM],
        out_specs=VM,
        scratch_shapes=[
            pltpu.VMEM((2, BEAMS, every), BF16),
            pltpu.VMEM((2 * share * count, every), BF16),
            pltpu.SemaphoreType.DMA((BEAMS // SPAN, 2)),
        ],
        compiler_params=params(MOST),
        cost_estimate=cost(2 * 2 * BEAMS * every * 2 * share * count),
        name="first_beams",
    )(first, beam_weights)
    powers = pl.pallas_call(
        last_beams_kernel,
        out_shape=jax.ShapeDtypeStruct((groups, share, 2 * mine), BF16),
        in_specs=[VM, HBM, VM, VM],
        out_specs=VM,
        scratch_shapes=[
            pltpu.VMEM((2, BEAMS, every), BF16),
            pltpu.VMEM((64 * LATE, every), BF16),
            pltpu.VMEM((64 * LATE, every), BF16),
            pltpu.VMEM((BLOCK, 128), F32),
            pltpu.VMEM((BEAMS // 128, share, 128), F32),
            pltpu.SemaphoreType.DMA((BEAMS // SPAN, 2)),
        ],
        compiler_params=params(WHOLE - (2 << 20)),
        cost_estimate=cost(2 * 2 * BEAMS * every * 2 * share * LATE),
        name="last_beams",
    )(second, beam_weights, partial, beam_order.reshape(BEAMS // 128, 128))
    owned = exchange(powers)
    filtered = pl.pallas_call(
        filter_kernel,
        out_shape=jax.ShapeDtypeStruct((mine, CHANNELS), F32),
        in_specs=[VM] * 3,
        out_specs=HBM,
        scratch_shapes=[
            pltpu.VMEM((mine, CHANNELS), F32),
            pltpu.SemaphoreType.DMA((2,)),
        ],
        compiler_params=params(20 * mib),
        cost_estimate=cost(4 * LIVE * CHANNELS * 2 * mine),
        name="filter",
    )(owned.reshape(LIVE, 2 * mine), filter_high, filter_low)
    return filtered.reshape(1, mine, CHANNELS)


def solution(mesh):
    placed = (P("feed", "tm"), P(None, "feed", None), P(), P(), P(), P())
    return jax.shard_map(
        stages, mesh=mesh, in_specs=placed, out_specs=P("tm", "feed", None), check_vma=False
    )
```
